32 devices in a mesh: subj: 4 (over y, core), vox: 8 (over z, x).
Axes of the slice: x: 2, y: 2, z: 4, core: 2. Of those that a mesh axis runs over, the one named last changes fastest.
Arguments:
- series: bfloat16 [16, 256, 16384], P('subj', None, 'vox'), may hold values from -6 to 6
- offsets: int32 [16, 12], replicated, may hold values from 0 to 240
- selected: int32 [16], replicated, may hold values from 0 to 16383, as said below
Outputs:
- kernel: float32 [16, 192, 192], P('vox', 'subj')
The draws below stay inside these ranges and needn't reach their ends.
Inputs may be any that keep to these rules, and one draw needn't show every extreme that they name: `offsets`: each epoch lies inside its subject's run; epochs may intersect. `selected`: the ids are distinct.
All inputs are finite; a program needn't handle non-finite values.
Results may differ from the reference program's by a relative error of at most 0.00035.
Values may be sent and summed in bfloat16 or wider, within the bound.
A program may use at most 128 MiB of HBM per device.

```python
import jax
import jax.numpy as jnp
from jax import lax

VOX = 16384
TR = 16
EP = 12
RUN_TR = 256
SUBJECTS = 16
SEL = 16


def draw_selected(key, part):
    first_key = jax.random.fold_in(key, 11)
    second_key = jax.random.fold_in(key, 12)
    middle = jax.random.permutation(first_key, VOX - 2)[:SEL - 2] + 1
    ends = jnp.array([0, VOX - 1], dtype=jnp.int32)
    joined = jnp.concatenate([ends, middle.astype(jnp.int32)])
    return jax.random.permutation(second_key, joined).astype(jnp.int32)


def plant(entries, stream_key, least, high):
    extent = entries.shape
    place = [jax.random.randint(jax.random.fold_in(stream_key, axis), (), 0, extent[axis]) for axis in range(len(extent))]
    entries = entries.at[tuple(place)].set(least)
    longest = extent.index(max(extent))
    place[longest] = (place[longest] + 1) % extent[longest]
    return entries.at[tuple(place)].set(high)


def block_levels(key, shape, cuts, smallest, top_value):
    def one(position, parts):
        steps = jax.random.uniform(jax.random.fold_in(jax.random.fold_in(key, 6), position), (parts,), jnp.float32, smallest / len(cuts), top_value / len(cuts))
        return jnp.repeat(jnp.exp(steps), shape[position] // parts).reshape((-1,) + (1,) * (len(shape) - position - 1))

    gain = one(*cuts[0])
    for cut in cuts[1:]:
        gain = gain * one(*cut)
    return gain


def bell_draw(key, dims, scale, reach, cuts=(), held_as=jnp.bfloat16):
    entries = scale * jax.random.normal(key, dims, jnp.float32)
    if cuts:
        entries = entries * block_levels(key, dims, cuts, -0.22, 0.18)
    return jnp.clip(entries, -reach, reach).astype(held_as)


def setup_inputs(seed: int = 0) -> dict:
    keys = jax.random.split(jax.random.key(seed), 4)
    return {
        "series": bell_draw(keys[0], (SUBJECTS, RUN_TR, VOX), 1.0, 6.0, ((0, 4), (2, 8))),
        "offsets": plant(jax.random.randint(keys[1], (SUBJECTS, EP), 0, RUN_TR - TR + 1), jax.random.fold_in(keys[1], 1), 0, RUN_TR - TR).astype(jnp.int32),
        "selected": draw_selected(jax.random.fold_in(keys[3], 71), 0),
    }


series_floor = 1.0
spread_floor = 0.05
shrink_factor = 0.9

def windows(block, starts):

    def subject_windows(subject_row, subject_offsets):
        return jax.vmap(lambda offset: lax.dynamic_slice_in_dim(subject_row, offset, TR, 0))(subject_offsets)
    return jax.vmap(subject_windows)(block, starts)

def standardize(values):
    centred = values - lax.optimization_barrier(jnp.mean(values, axis=2, keepdims=True))
    return centred / jnp.sqrt(lax.optimization_barrier(jnp.sum(centred * centred, axis=2, keepdims=True)) + series_floor)

def fisher_transform(correlation):
    shrunk = shrink_factor * correlation
    return 0.5 * jnp.log((1.0 + shrunk) / (1.0 - shrunk))

def scores(slab_std, voxel_std):
    correlation = jnp.einsum('setk,setv->ksev', slab_std, voxel_std, precision=lax.Precision.HIGHEST)
    fisher = fisher_transform(correlation)
    centred = fisher - lax.optimization_barrier(jnp.mean(fisher, axis=2, keepdims=True))
    variance = lax.optimization_barrier(jnp.mean(centred * centred, axis=2, keepdims=True))
    zscored = (centred / jnp.sqrt(variance + spread_floor)).astype(jnp.bfloat16)
    return zscored.reshape(zscored.shape[0], zscored.shape[1] * zscored.shape[2], zscored.shape[3])

def reference(series, offsets, selected):
    epochs = windows(series, offsets)
    voxel_std = standardize(epochs.astype(jnp.float32))
    slab_std = standardize(jnp.take(epochs, selected, axis=3).astype(jnp.float32))
    block_width = 8
    blocks = jnp.moveaxis(slab_std.reshape(slab_std.shape[:3] + (SEL // block_width, block_width)), 3, 0)

    def kernel_block(slab_block):
        zscored = scores(slab_block, voxel_std).astype(jnp.float32)
        return jnp.einsum('kev,kfv->kef', zscored, zscored, precision=lax.Precision.HIGHEST) * (1.0 / VOX)
    mapped = lax.map(kernel_block, blocks)
    return mapped.reshape(SEL, mapped.shape[2], mapped.shape[3])
```

```python
import functools

import jax
import jax.numpy as jnp
from jax import lax
from jax.experimental import pallas as pl
from jax.experimental.pallas import tpu as pltpu
from jax.sharding import PartitionSpec as P

TR = 16
KB = 8
series_floor = 1.0
spread_floor = 0.05
shrink_factor = 0.9
f32 = jnp.float32
bf16 = jnp.bfloat16


def iota(shape, dim):
    return lax.broadcasted_iota(jnp.int32, shape, dim)


def kernel(
    G, V, NS, EP, SEL, W,
    off_ref, sel_ref, series_ref, out_ref,
    ep, inv, part, slots, a_hi, a_lo, perm, send, recv, gram, rsbuf,
    slab_send, slab_recv, sc_send, sc_recv, rs_send, rs_recv,
):
    subj = lax.axis_index("subj")
    vox = lax.axis_index("vox")
    RUN = series_ref.shape[1]
    VL = series_ref.shape[2]
    ROWS = EP * TR
    H = SEL // KB
    KH = KB // G
    SL = SEL // V
    NE = NS * EP
    chunks = VL // W

    barrier = pltpu.get_barrier_semaphore()
    for dj in range(G):
        for dv in range(V):
            if dj or dv:
                pl.semaphore_signal(
                    barrier, inc=1,
                    device_id=(lax.rem(subj + dj, G), lax.rem(vox + dv, V)),
                    device_id_type=pl.DeviceIdType.MESH,
                )

    for s in range(NS):
        col = iota((TR, RUN), 1)
        row = iota((TR, RUN), 0)
        tiles = [
            jnp.where(col == row + off_ref[subj * NS + s, e], 1.0, 0.0) for e in range(EP)
        ]
        hot = jnp.concatenate(tiles, axis=0).astype(bf16)

        def gather(c, carry, hot=hot, s=s):
            at = pl.ds(pl.multiple_of(c * W, W), W)
            x = jnp.dot(hot, series_ref[s, :, at], preferred_element_type=f32)
            ep[s, :, at] = x.astype(bf16)
            x3 = x.reshape(EP, TR, W)
            total = jnp.sum(x3, axis=1)
            ssq = jnp.sum(x3 * x3, axis=1) - total * total * (1.0 / TR)
            inv[s, :, at] = shrink_factor * lax.rsqrt(jnp.maximum(ssq, 0.0) + series_floor)
            return carry

        lax.fori_loop(0, chunks, gather, 0)

    ids = jnp.zeros((SEL, 1), jnp.int32)
    which = iota((SEL, 1), 0)
    for p in range(SEL):
        ids = jnp.where(which == p, sel_ref[(p % V) * SL + p // V], ids)
    picker = jnp.where(iota((SEL, VL), 1) + vox * VL == ids, 1.0, 0.0).astype(bf16)
    for s in range(NS):
        got = lax.dot_general(
            picker, ep[s], (((1,), (1,)), ((), ())), preferred_element_type=f32
        )
        part[s] = got.astype(bf16)

    pl.semaphore_wait(barrier, G * V - 1)

    def slab_copy(d, sender):
        return pltpu.make_async_remote_copy(
            src_ref=part, dst_ref=slots.at[sender],
            send_sem=slab_send.at[d], recv_sem=slab_recv.at[d],
            device_id=(subj, lax.rem(vox + d, V)),
            device_id_type=pl.DeviceIdType.MESH,
        )

    for d in range(1, V):
        slab_copy(d, vox).start()

    out_row = iota((KB * NE, KB * NE), 0)
    in_row = iota((KB * NE, KB * NE), 1)
    source = lax.rem(out_row, NE) * KB + out_row // NE
    perm[...] = jnp.where(source == in_row, 1.0, 0.0).astype(bf16)

    for d in range(1, V):
        slab_copy(d, lax.rem(vox - d + V, V)).wait_recv()

    same = iota((ROWS, ROWS), 0) // TR == iota((ROWS, ROWS), 1) // TR
    ones = jnp.where(same, 1.0, 0.0)
    pick_e = iota((EP, KB, ROWS), 2) // TR == iota((EP, KB, ROWS), 0)
    for s in range(NS):
        slab = part[s].astype(f32)
        for d in range(1, V):
            slab = slab + slots[lax.rem(vox + d, V), s].astype(f32)
        mean = jnp.dot(
            slab, ones, precision=lax.Precision.HIGHEST, preferred_element_type=f32
        ) * (1.0 / TR)
        centred = slab - mean
        ssq = jnp.dot(
            centred * centred, ones,
            precision=lax.Precision.HIGHEST, preferred_element_type=f32,
        )
        std = centred / jnp.sqrt(ssq + series_floor)
        hi = std.astype(bf16).astype(f32)
        lo = std - hi
        for h in range(H):
            for value, where in ((hi, a_hi), (lo, a_lo)):
                block = value[h * KB:(h + 1) * KB]
                spread = jnp.where(pick_e, block[None], 0.0).reshape(EP * KB, ROWS)
                where[h, s] = spread.astype(bf16)

    def score_copy(h, d, sender, at):
        return pltpu.make_async_remote_copy(
            src_ref=send.at[h, lax.rem(subj + d, G), :, :, at],
            dst_ref=recv.at[h, :, pl.ds(pl.multiple_of(sender * NE, NE), NE), at],
            send_sem=sc_send.at[h, d], recv_sem=sc_recv.at[h, d],
            device_id=(lax.rem(subj + d, G), vox),
            device_id_type=pl.DeviceIdType.MESH,
        )

    own_rows = pl.ds(pl.multiple_of(subj * NE, NE), NE)
    for h in range(H):
        def scores(c, carry, h=h):
            at = pl.ds(pl.multiple_of(c * W, W), W)
            parts = []
            for s in range(NS):
                x = ep[s, :, at]
                corr = jnp.dot(a_hi[h, s], x, preferred_element_type=f32)
                corr = corr + jnp.dot(a_lo[h, s], x, preferred_element_type=f32)
                r = corr.reshape(EP, KB, W) * inv[s, :, at][:, None, :]
                f = 0.5 * (jnp.log(1.0 + r) - jnp.log(1.0 - r))
                f = f - jnp.sum(f, axis=0, keepdims=True) * (1.0 / EP)
                var = jnp.sum(f * f, axis=0, keepdims=True) * (1.0 / EP)
                z = f * lax.rsqrt(var + spread_floor)
                parts.append(z.reshape(EP * KB, W).astype(bf16))
            z = jnp.concatenate(parts, axis=0)
            moved = jnp.dot(perm[...], z, preferred_element_type=f32)
            send[h, :, :, :, at] = moved.astype(bf16).reshape(G, KH, NE, W)
            for d in range(1, G):
                score_copy(h, d, subj, at).start()
            recv[h, :, own_rows, at] = send[h, subj, :, :, at]
            return carry

        lax.fori_loop(0, chunks, scores, 0)

    whole = pl.ds(0, VL)

    def rs_copy(h, i, dj, owner, local):
        to = lax.rem(subj + dj, G)
        return pltpu.make_async_remote_copy(
            src_ref=gram.at[h, i, pl.ds(pl.multiple_of(to * NE, NE), NE)],
            dst_ref=rsbuf.at[local, vox],
            send_sem=rs_send.at[h, i, dj], recv_sem=rs_recv.at[local, vox],
            device_id=(to, owner),
            device_id_type=pl.DeviceIdType.MESH,
        )

    def spot(h, i):
        p = h * KB + subj * KH + i
        return lax.rem(p, V), p // V

    for h in range(H):
        for d in range(1, G):
            score_copy(h, d, lax.rem(subj - d + G, G), whole).wait_recv()
        for i in range(KH):
            rows = recv[h, i]
            gram[h, i] = lax.dot_general(
                rows, rows, (((1,), (1,)), ((), ())), preferred_element_type=f32
            )
            owner, local = spot(h, i)
            for dj in range(G):
                if dj:
                    rs_copy(h, i, dj, owner, local).start()
                else:
                    @pl.when(owner != vox)
                    def _():
                        rs_copy(h, i, 0, owner, local).start()

                    @pl.when(owner == vox)
                    def _():
                        rsbuf[local, vox] = gram[h, i, own_rows]

    for local in range(SL):
        p = local * V + vox
        handler = lax.rem(p, KB) // KH
        total = None
        for v in range(V):
            @pl.when(jnp.logical_or(handler != subj, vox != v))
            def _():
                pltpu.make_async_remote_copy(
                    src_ref=gram.at[0, 0, pl.ds(0, NE)],
                    dst_ref=rsbuf.at[local, v],
                    send_sem=rs_send.at[0, 0, 0], recv_sem=rs_recv.at[local, v],
                    device_id=(subj, lax.rem(vox + 1, V)),
                    device_id_type=pl.DeviceIdType.MESH,
                ).wait_recv()
            term = rsbuf[local, v]
            total = term if total is None else total + term
        out_ref[local] = total * (1.0 / (VL * V))

    for d in range(1, V):
        slab_copy(d, vox).wait_send()
    for h in range(H):
        for d in range(1, G):
            score_copy(h, d, subj, whole).wait_send()
        for i in range(KH):
            owner, local = spot(h, i)
            for dj in range(G):
                if dj:
                    rs_copy(h, i, dj, owner, local).wait_send()
                else:
                    @pl.when(owner != vox)
                    def _():
                        rs_copy(h, i, 0, owner, local).wait_send()


def body(series, offsets, selected):
    G = lax.axis_size("subj")
    V = lax.axis_size("vox")
    NS, RUN, VL = series.shape
    EP = offsets.shape[1]
    SEL = selected.shape[0]
    W = 256
    NE = NS * EP
    ROWS = EP * TR
    H = SEL // KB
    KH = KB // G
    SL = SEL // V
    vm = pltpu.VMEM
    dma = pltpu.SemaphoreType.DMA
    return pl.pallas_call(
        functools.partial(kernel, G, V, NS, EP, SEL, W),
        out_shape=jax.ShapeDtypeStruct((SL, NE, G * NE), f32),
        in_specs=[
            pl.BlockSpec(memory_space=pltpu.SMEM),
            pl.BlockSpec(memory_space=pltpu.SMEM),
            pl.BlockSpec(memory_space=pltpu.VMEM),
        ],
        out_specs=pl.BlockSpec(memory_space=pltpu.VMEM),
        scratch_shapes=[
            vm((NS, ROWS, VL), bf16),
            vm((NS, EP, VL), f32),
            vm((NS, SEL, ROWS), bf16),
            vm((V, NS, SEL, ROWS), bf16),
            vm((H, NS, EP * KB, ROWS), bf16),
            vm((H, NS, EP * KB, ROWS), bf16),
            vm((KB * NE, KB * NE), bf16),
            vm((H, G, KH, NE, VL), bf16),
            vm((H, KH, G * NE, VL), bf16),
            vm((H, KH, G * NE, G * NE), f32),
            vm((SL, V, NE, G * NE), f32),
            dma((V,)),
            dma((V,)),
            dma((H, G)),
            dma((H, G)),
            dma((H, KH, G)),
            dma((SL, V)),
        ],
        compiler_params=pltpu.CompilerParams(
            collective_id=0, has_side_effects=True, vmem_limit_bytes=56 * 1024 * 1024
        ),
    )(offsets, selected, series)


def solution(mesh):
    placed = (P("subj", None, "vox"), P(), P())
    return jax.shard_map(
        body, mesh=mesh, in_specs=placed, out_specs=P("vox", "subj", None), check_vma=False
    )
```

```python
import functools

import jax
import jax.numpy as jnp
from jax import lax
from jax.experimental import pallas as pl
from jax.experimental.pallas import tpu as pltpu
from jax.sharding import PartitionSpec as P

TR = 16
KB = 8
series_floor = 1.0
spread_floor = 0.05
shrink_factor = 0.9
f32 = jnp.float32
bf16 = jnp.bfloat16


def iota(shape, dim):
    return lax.broadcasted_iota(jnp.int32, shape, dim)


def pieces_of(G, V, NE):
    R = V
    while R > G and (V % R or R % G or (G * NE) % R or (G * NE // R) % 8):
        R -= 1
    return R


def kernel(
    G, V, NS, EP, SEL, W,
    off_ref, sel_ref, series_ref, out_ref,
    ep, hot, inv, part, slots, a_hi, a_lo, perm, send, recv,
    gram, pieces_in, summed, landed,
    slab_send, slab_recv, sc_send, sc_recv, rs_send, rs_recv, fin_send, fin_recv,
):
    subj = lax.axis_index("subj")
    vox = lax.axis_index("vox")
    RUN = series_ref.shape[1]
    VL = series_ref.shape[2]
    ROWS = EP * TR
    H = SEL // KB
    KH = KB // G
    SL = SEL // V
    NE = NS * EP
    chunks = VL // W
    R = pieces_of(G, V, NE)
    VR = V // R
    RP = G * NE // R
    PG = R // G
    ORDER = tuple(range(G // 2, G)) + tuple(range(1, G // 2))

    barrier = pltpu.get_barrier_semaphore()
    for dj in range(G):
        for dv in range(V):
            if dj or dv:
                pl.semaphore_signal(
                    barrier, inc=1,
                    device_id=(lax.rem(subj + dj, G), lax.rem(vox + dv, V)),
                    device_id_type=pl.DeviceIdType.MESH,
                )

    ids = jnp.zeros((SEL, 1), jnp.int32)
    which = iota((SEL, 1), 0)
    for p in range(SEL):
        ids = jnp.where(which == p, sel_ref[(p % V) * SL + p // V], ids)
    picker = jnp.where(iota((SEL, VL), 1) + vox * VL == ids, 1.0, 0.0).astype(bf16)
    col = iota((TR, RUN), 1) - iota((TR, RUN), 0)
    pieces = []
    for s in range(NS):
        tiles = [
            jnp.where(col == off_ref[subj * NS + s, e], 1.0, 0.0) for e in range(EP)
        ]
        hot[s] = jnp.concatenate(tiles, axis=0).astype(bf16)
        runs = lax.dot_general(
            picker, series_ref[s], (((1,), (1,)), ((), ())), preferred_element_type=f32
        )
        pieces.append(lax.dot_general(
            runs.astype(bf16), hot[s], (((1,), (1,)), ((), ())), preferred_element_type=f32
        ))
    joined = jnp.concatenate(pieces, axis=1)
    for h in range(H):
        part[h] = joined[h * KB:(h + 1) * KB].astype(bf16)

    pl.semaphore_wait(barrier, G * V - 1)

    def slab_copy(h, d, sender):
        return pltpu.make_async_remote_copy(
            src_ref=part.at[h], dst_ref=slots.at[h, sender],
            send_sem=slab_send.at[h, d], recv_sem=slab_recv.at[h, d],
            device_id=(subj, lax.rem(vox + d, V)),
            device_id_type=pl.DeviceIdType.MESH,
        )

    for h in range(H):
        for d in range(1, V):
            slab_copy(h, d, vox).start()

    def gather(c, carry):
        at = pl.ds(pl.multiple_of(c * W, W), W)
        for s in range(NS):
            x = jnp.dot(hot[s], series_ref[s, :, at], preferred_element_type=f32)
            ep[s, :, at] = x.astype(bf16)
            x3 = x.reshape(EP, TR, W)
            total = jnp.sum(x3, axis=1)
            ssq = jnp.sum(x3 * x3, axis=1) - total * total * (1.0 / TR)
            inv[s, :, at] = shrink_factor * lax.rsqrt(jnp.maximum(ssq, 0.0) + series_floor)
        return carry

    lax.fori_loop(0, chunks, gather, 0)

    out_row = iota((KB * NE, KB * NE), 0)
    in_row = iota((KB * NE, KB * NE), 1)
    slot = out_row // NE
    source = lax.rem(out_row, NE) * KB + lax.rem(slot, KH) * G + slot // KH
    perm[...] = jnp.where(source == in_row, 1.0, 0.0).astype(bf16)

    same = iota((ROWS, ROWS), 0) // TR == iota((ROWS, ROWS), 1) // TR
    ones = jnp.where(same, 1.0, 0.0)
    pick_e = iota((EP, KB, ROWS), 2) // TR == iota((EP, KB, ROWS), 0)

    def slab_rows(h):
        slab = part[h].astype(f32)
        for d in range(1, V):
            slab_copy(h, d, lax.rem(vox - d + V, V)).wait_recv()
        for d in range(1, V):
            slab = slab + slots[h, lax.rem(vox + d, V)].astype(f32)
        rows = jnp.concatenate(
            [slab[:, s * ROWS:(s + 1) * ROWS] for s in range(NS)], axis=0
        )
        mean = jnp.dot(
            rows.astype(bf16), ones.astype(bf16), preferred_element_type=f32
        ) * (1.0 / TR)
        centred = rows - mean
        ssq = jnp.dot(
            centred * centred, ones,
            precision=lax.Precision.HIGHEST, preferred_element_type=f32,
        )
        std = centred / jnp.sqrt(ssq + series_floor)
        hi = std.astype(bf16).astype(f32)
        lo = std - hi
        for s in range(NS):
            for value, where in ((hi, a_hi), (lo, a_lo)):
                block = value[s * KB:(s + 1) * KB]
                spread = jnp.where(pick_e, block[None], 0.0).reshape(EP * KB, ROWS)
                where[h, s] = spread.astype(bf16)

    every = pl.ds(0, VL)

    def score_copy(h, i, n, d, sender, at):
        return pltpu.make_async_remote_copy(
            src_ref=send.at[h, lax.rem(subj + d, G), pl.ds(i, n), :, at],
            dst_ref=recv.at[h, pl.ds(i, n), pl.ds(pl.multiple_of(sender * NE, NE), NE), at],
            send_sem=sc_send.at[h, i, d], recv_sem=sc_recv.at[h, i, d],
            device_id=(lax.rem(subj + d, G), vox),
            device_id_type=pl.DeviceIdType.MESH,
        )

    def groups(h):
        return ((0, KH),) if h == 0 else tuple((i, 1) for i in range(KH))

    own_rows = pl.ds(pl.multiple_of(subj * NE, NE), NE)
    for h in range(H):
        slab_rows(h)

        def scores(c, carry, h=h):
            at = pl.ds(pl.multiple_of(c * W, W), W)
            parts = []
            for s in range(NS):
                x = ep[s, :, at]
                corr = jnp.dot(a_hi[h, s], x, preferred_element_type=f32)
                corr = corr + jnp.dot(a_lo[h, s], x, preferred_element_type=f32)
                r = corr.reshape(EP, KB, W) * inv[s, :, at][:, None, :]
                f = 0.5 * (jnp.log(1.0 + r) - jnp.log(1.0 - r))
                f = f - jnp.sum(f, axis=0, keepdims=True) * (1.0 / EP)
                var = jnp.sum(f * f, axis=0, keepdims=True) * (1.0 / EP)
                z = f * lax.rsqrt(var + spread_floor)
                parts.append(z.reshape(EP * KB, W).astype(bf16))
            z = jnp.concatenate(parts, axis=0)
            moved = jnp.dot(perm[...], z, preferred_element_type=f32)
            send[h, :, :, :, at] = moved.astype(bf16).reshape(G, KH, NE, W)
            if h == 0:
                for d in ORDER:
                    score_copy(h, 0, KH, d, subj, at).start()
            recv[h, :, own_rows, at] = send[h, subj, :, :, at]
            return carry

        lax.fori_loop(0, chunks, scores, 0)

        if h:
            for i, n in groups(h):
                for d in ORDER:
                    score_copy(h, i, n, d, subj, every).start()

    def row_piece(r):
        return pl.ds(pl.multiple_of(r * RP, RP), RP)

    def part_copy(t, d):
        to = lax.rem(vox + d, V)
        return pltpu.make_async_remote_copy(
            src_ref=gram.at[t, row_piece(to // VR)], dst_ref=pieces_in.at[t, d - 1],
            send_sem=rs_send.at[t, d], recv_sem=rs_recv.at[t],
            device_id=(subj, to), device_id_type=pl.DeviceIdType.MESH,
        )

    def all_parts(t):
        return pltpu.make_async_remote_copy(
            src_ref=pieces_in.at[t], dst_ref=pieces_in.at[t],
            send_sem=rs_send.at[t, 0], recv_sem=rs_recv.at[t],
            device_id=(subj, lax.rem(vox + 1, V)), device_id_type=pl.DeviceIdType.MESH,
        )

    piece = vox // VR
    to_subj = piece // PG
    to_rows = lax.rem(piece, PG)

    def reduces(v):
        return lax.rem(v, VR) == 0

    def spot(t):
        p = t * G + subj
        return lax.rem(p, V), p // V

    def final_copy(t):
        owner, local = spot(t)
        return pltpu.make_async_remote_copy(
            src_ref=summed.at[t], dst_ref=landed.at[local, to_rows],
            send_sem=fin_send.at[t], recv_sem=fin_recv.at[local, to_rows],
            device_id=(to_subj, owner), device_id_type=pl.DeviceIdType.MESH,
        )

    def away(t):
        owner, local = spot(t)
        return jnp.logical_or(to_subj != subj, owner != vox)

    def finish(t):
        @pl.when(reduces(vox))
        def _():
            all_parts(t).wait_recv()
            total = gram[t, row_piece(piece)]
            for d in range(1, V):
                total = total + pieces_in[t, d - 1]
            total = total * (1.0 / (VL * V))
            summed[t] = total

            @pl.when(away(t))
            def _():
                final_copy(t).start()

            @pl.when(jnp.logical_not(away(t)))
            def _():
                landed[spot(t)[1], to_rows] = total

    T = H * KH
    for h in range(H):
        for i in range(KH):
            t = h * KH + i
            for first, n in groups(h):
                if first == i:
                    for d in range(1, G):
                        sender = lax.rem(subj - d + G, G)
                        score_copy(h, i, n, d, sender, every).wait_recv()
            rows = recv[h, i]
            gram[t] = lax.dot_general(
                rows, rows, (((1,), (1,)), ((), ())), preferred_element_type=f32
            )
            for d in range(1, V):
                @pl.when(reduces(lax.rem(vox + d, V)))
                def _():
                    part_copy(t, d).start()
            if t:
                finish(t - 1)
    finish(T - 1)

    for local in range(SL):
        p = local * V + vox
        handler = lax.rem(p, G)
        for b in range(PG):
            source = (subj * PG + b) * VR

            @pl.when(jnp.logical_or(handler != subj, source != vox))
            def _():
                pltpu.make_async_remote_copy(
                    src_ref=summed.at[0], dst_ref=landed.at[local, b],
                    send_sem=fin_send.at[0], recv_sem=fin_recv.at[local, b],
                    device_id=(subj, lax.rem(vox + 1, V)),
                    device_id_type=pl.DeviceIdType.MESH,
                ).wait_recv()
            out_ref[local, b * RP:(b + 1) * RP] = landed[local, b]

    for h in range(H):
        for d in range(1, V):
            slab_copy(h, d, vox).wait_send()
        for i, n in groups(h):
            for d in range(1, G):
                score_copy(h, i, n, d, subj, every).wait_send()
    for t in range(T):
        for d in range(1, V):
            @pl.when(reduces(lax.rem(vox + d, V)))
            def _():
                part_copy(t, d).wait_send()

        @pl.when(jnp.logical_and(reduces(vox), away(t)))
        def _():
            final_copy(t).wait_send()


def body(series, offsets, selected):
    G = lax.axis_size("subj")
    V = lax.axis_size("vox")
    NS, RUN, VL = series.shape
    EP = offsets.shape[1]
    SEL = selected.shape[0]
    W = 256
    NE = NS * EP
    ROWS = EP * TR
    H = SEL // KB
    KH = KB // G
    SL = SEL // V
    R = pieces_of(G, V, NE)
    RP = G * NE // R
    vm = pltpu.VMEM
    dma = pltpu.SemaphoreType.DMA
    return pl.pallas_call(
        functools.partial(kernel, G, V, NS, EP, SEL, W),
        out_shape=jax.ShapeDtypeStruct((SL, NE, G * NE), f32),
        in_specs=[
            pl.BlockSpec(memory_space=pltpu.SMEM),
            pl.BlockSpec(memory_space=pltpu.SMEM),
            pl.BlockSpec(memory_space=pltpu.VMEM),
        ],
        out_specs=pl.BlockSpec(memory_space=pltpu.VMEM),
        scratch_shapes=[
            vm((NS, ROWS, VL), bf16),
            vm((NS, ROWS, RUN), bf16),
            vm((NS, EP, VL), f32),
            vm((H, KB, NS * ROWS), bf16),
            vm((H, V, KB, NS * ROWS), bf16),
            vm((H, NS, EP * KB, ROWS), bf16),
            vm((H, NS, EP * KB, ROWS), bf16),
            vm((KB * NE, KB * NE), bf16),
            vm((H, G, KH, NE, VL), bf16),
            vm((H, KH, G * NE, VL), bf16),
            vm((H * KH, G * NE, G * NE), f32),
            vm((H * KH, V - 1, RP, G * NE), f32),
            vm((H * KH, RP, G * NE), f32),
            vm((SL, R // G, RP, G * NE), f32),
            dma((H, V)),
            dma((H, V)),
            dma((H, KH, G)),
            dma((H, KH, G)),
            dma((H * KH, V)),
            dma((H * KH,)),
            dma((H * KH,)),
            dma((SL, R // G)),
        ],
        compiler_params=pltpu.CompilerParams(
            collective_id=0, has_side_effects=True, vmem_limit_bytes=56 * 1024 * 1024
        ),
    )(offsets, selected, series)


def solution(mesh):
    placed = (P("subj", None, "vox"), P(), P())
    return jax.shard_map(
        body, mesh=mesh, in_specs=placed, out_specs=P("vox", "subj", None), check_vma=False
    )
```

```python
import functools

import jax
import jax.numpy as jnp
from jax import lax
from jax.experimental import pallas as pl
from jax.experimental.pallas import tpu as pltpu
from jax.sharding import PartitionSpec as P

TR = 16
KB = 8
series_floor = 1.0
spread_floor = 0.05
shrink_factor = 0.9
f32 = jnp.float32
bf16 = jnp.bfloat16


def iota(shape, dim):
    return lax.broadcasted_iota(jnp.int32, shape, dim)


def pieces_of(G, V, NE):
    R = V
    while R > G and (V % R or R % G or (G * NE) % R or (G * NE // R) % 8):
        R -= 1
    return R


def kernel(
    G, V, NS, EP, SEL, W,
    off_ref, sel_ref, series_hbm, out_ref,
    series_ref, load_sem, ep, hot, inv, part, slots, a_hi, a_lo, perm, send, recv,
    gram, pieces_in, summed, landed,
    slab_send, slab_recv, sc_send, sc_recv, rs_send, rs_recv, fin_send, fin_recv,
):
    subj = lax.axis_index("subj")
    vox = lax.axis_index("vox")
    RUN = series_ref.shape[1]
    VL = series_ref.shape[2]
    ROWS = EP * TR
    H = SEL // KB
    KH = KB // G
    SL = SEL // V
    NE = NS * EP
    chunks = VL // W
    R = pieces_of(G, V, NE)
    VR = V // R
    RP = G * NE // R
    PG = R // G
    ORDER = tuple(range(G // 2, G)) + tuple(range(1, G // 2))

    barrier = pltpu.get_barrier_semaphore()
    for d in range(1, G):
        pl.semaphore_signal(
            barrier, inc=1, device_id=(lax.rem(subj + d, G), vox),
            device_id_type=pl.DeviceIdType.MESH,
        )
    for d in range(1, V):
        pl.semaphore_signal(
            barrier, inc=1, device_id=(subj, lax.rem(vox + d, V)),
            device_id_type=pl.DeviceIdType.MESH,
        )

    def load(s):
        return pltpu.make_async_copy(series_hbm.at[s], series_ref.at[s], load_sem.at[s])

    for s in range(NS):
        load(s).start()

    ids = jnp.zeros((SEL, 1), jnp.int32)
    which = iota((SEL, 1), 0)
    for p in range(SEL):
        ids = jnp.where(which == p, sel_ref[(p % V) * SL + p // V], ids)
    picker = jnp.where(iota((SEL, VL), 1) + vox * VL == ids, 1.0, 0.0).astype(bf16)
    col = iota((TR, RUN), 1) - iota((TR, RUN), 0)
    pieces = []
    for s in range(NS):
        tiles = [
            jnp.where(col == off_ref[subj * NS + s, e], 1.0, 0.0) for e in range(EP)
        ]
        hot[s] = jnp.concatenate(tiles, axis=0).astype(bf16)
        load(s).wait()
        runs = lax.dot_general(
            picker, series_ref[s], (((1,), (1,)), ((), ())), preferred_element_type=f32
        )
        pieces.append(lax.dot_general(
            runs.astype(bf16), hot[s], (((1,), (1,)), ((), ())), preferred_element_type=f32
        ))
    joined = jnp.concatenate(pieces, axis=1)
    for h in range(H):
        part[h] = joined[h * KB:(h + 1) * KB].astype(bf16)

    pl.semaphore_wait(barrier, G + V - 2)

    def slab_copy(h, d, sender):
        return pltpu.make_async_remote_copy(
            src_ref=part.at[h], dst_ref=slots.at[h, sender],
            send_sem=slab_send.at[h, d], recv_sem=slab_recv.at[h, d],
            device_id=(subj, lax.rem(vox + d, V)),
            device_id_type=pl.DeviceIdType.MESH,
        )

    for h in range(H):
        for d in range(1, V):
            slab_copy(h, d, vox).start()

    def gather(c, carry):
        at = pl.ds(pl.multiple_of(c * W, W), W)
        for s in range(NS):
            x = jnp.dot(hot[s], series_ref[s, :, at], preferred_element_type=f32)
            ep[s, :, at] = x.astype(bf16)
            x3 = x.reshape(EP, TR, W)
            total = jnp.sum(x3, axis=1)
            ssq = jnp.sum(x3 * x3, axis=1) - total * total * (1.0 / TR)
            inv[s, :, at] = shrink_factor * lax.rsqrt(jnp.maximum(ssq, 0.0) + series_floor)
        return carry

    lax.fori_loop(0, chunks, gather, 0)

    out_row = iota((KB * NE, KB * NE), 0)
    in_row = iota((KB * NE, KB * NE), 1)
    slot = out_row // NE
    source = lax.rem(out_row, NE) * KB + lax.rem(slot, KH) * G + slot // KH
    perm[...] = jnp.where(source == in_row, 1.0, 0.0).astype(bf16)

    same = iota((ROWS, ROWS), 0) // TR == iota((ROWS, ROWS), 1) // TR
    ones = jnp.where(same, 1.0, 0.0)
    pick_e = iota((EP, KB, ROWS), 2) // TR == iota((EP, KB, ROWS), 0)

    def slab_rows(h):
        slab = part[h].astype(f32)
        for d in range(1, V):
            slab_copy(h, d, lax.rem(vox - d + V, V)).wait_recv()
        for d in range(1, V):
            slab = slab + slots[h, lax.rem(vox + d, V)].astype(f32)
        rows = jnp.concatenate(
            [slab[:, s * ROWS:(s + 1) * ROWS] for s in range(NS)], axis=0
        )
        mean = jnp.dot(
            rows.astype(bf16), ones.astype(bf16), preferred_element_type=f32
        ) * (1.0 / TR)
        centred = rows - mean
        ssq = jnp.dot(
            centred * centred, ones,
            precision=lax.Precision.HIGHEST, preferred_element_type=f32,
        )
        std = centred / jnp.sqrt(ssq + series_floor)
        hi = std.astype(bf16).astype(f32)
        lo = std - hi
        for s in range(NS):
            for value, where in ((hi, a_hi), (lo, a_lo)):
                block = value[s * KB:(s + 1) * KB]
                spread = jnp.where(pick_e, block[None], 0.0).reshape(EP * KB, ROWS)
                where[h, s] = spread.astype(bf16)

    every = pl.ds(0, VL)

    def score_copy(h, i, n, d, sender, at):
        return pltpu.make_async_remote_copy(
            src_ref=send.at[h, lax.rem(subj + d, G), pl.ds(i, n), :, at],
            dst_ref=recv.at[h, pl.ds(i, n), pl.ds(pl.multiple_of(sender * NE, NE), NE), at],
            send_sem=sc_send.at[h, i, d], recv_sem=sc_recv.at[h, i, d],
            device_id=(lax.rem(subj + d, G), vox),
            device_id_type=pl.DeviceIdType.MESH,
        )

    def groups(h):
        return ((0, KH),) if h == 0 else tuple((i, 1) for i in range(KH))

    own_rows = pl.ds(pl.multiple_of(subj * NE, NE), NE)
    for h in range(H):
        slab_rows(h)

        def scores(c, carry, h=h):
            at = pl.ds(pl.multiple_of(c * W, W), W)
            parts = []
            for s in range(NS):
                x = ep[s, :, at]
                corr = jnp.dot(a_hi[h, s], x, preferred_element_type=f32)
                corr = corr + jnp.dot(a_lo[h, s], x, preferred_element_type=f32)
                r = corr.reshape(EP, KB, W) * inv[s, :, at][:, None, :]
                f = 0.5 * (jnp.log(1.0 + r) - jnp.log(1.0 - r))
                f = f - jnp.sum(f, axis=0, keepdims=True) * (1.0 / EP)
                var = jnp.sum(f * f, axis=0, keepdims=True) * (1.0 / EP)
                z = f * lax.rsqrt(var + spread_floor)
                parts.append(z.reshape(EP * KB, W).astype(bf16))
            z = jnp.concatenate(parts, axis=0)
            moved = jnp.dot(perm[...], z, preferred_element_type=f32)
            send[h, :, :, :, at] = moved.astype(bf16).reshape(G, KH, NE, W)
            if h == 0:
                for d in ORDER:
                    score_copy(h, 0, KH, d, subj, at).start()
            recv[h, :, own_rows, at] = send[h, subj, :, :, at]
            return carry

        lax.fori_loop(0, chunks, scores, 0)

        if h:
            for i, n in groups(h):
                for d in ORDER:
                    score_copy(h, i, n, d, subj, every).start()

    def row_piece(r):
        return pl.ds(pl.multiple_of(r * RP, RP), RP)

    def part_copy(t, d):
        to = lax.rem(vox + d, V)
        return pltpu.make_async_remote_copy(
            src_ref=gram.at[t, row_piece(to // VR)], dst_ref=pieces_in.at[t, d - 1],
            send_sem=rs_send.at[t, d], recv_sem=rs_recv.at[t],
            device_id=(subj, to), device_id_type=pl.DeviceIdType.MESH,
        )

    def all_parts(t):
        return pltpu.make_async_remote_copy(
            src_ref=pieces_in.at[t], dst_ref=pieces_in.at[t],
            send_sem=rs_send.at[t, 0], recv_sem=rs_recv.at[t],
            device_id=(subj, lax.rem(vox + 1, V)), device_id_type=pl.DeviceIdType.MESH,
        )

    piece = vox // VR
    to_subj = piece // PG
    to_rows = lax.rem(piece, PG)

    def reduces(v):
        return lax.rem(v, VR) == 0

    def spot(t):
        p = t * G + subj
        return lax.rem(p, V), p // V

    def final_copy(t):
        owner, local = spot(t)
        return pltpu.make_async_remote_copy(
            src_ref=summed.at[t], dst_ref=landed.at[local, to_rows],
            send_sem=fin_send.at[t], recv_sem=fin_recv.at[local, to_rows],
            device_id=(to_subj, owner), device_id_type=pl.DeviceIdType.MESH,
        )

    def away(t):
        owner, local = spot(t)
        return jnp.logical_or(to_subj != subj, owner != vox)

    def finish(t):
        @pl.when(reduces(vox))
        def _():
            all_parts(t).wait_recv()
            total = gram[t, row_piece(piece)]
            for d in range(1, V):
                total = total + pieces_in[t, d - 1]
            total = total * (1.0 / (VL * V))
            summed[t] = total

            @pl.when(away(t))
            def _():
                final_copy(t).start()

            @pl.when(jnp.logical_not(away(t)))
            def _():
                landed[spot(t)[1], to_rows] = total

    T = H * KH
    for h in range(H):
        for i in range(KH):
            t = h * KH + i
            for first, n in groups(h):
                if first == i:
                    for d in range(1, G):
                        sender = lax.rem(subj - d + G, G)
                        score_copy(h, i, n, d, sender, every).wait_recv()
            rows = recv[h, i]
            gram[t] = lax.dot_general(
                rows, rows, (((1,), (1,)), ((), ())), preferred_element_type=f32
            )
            for d in range(1, V):
                @pl.when(reduces(lax.rem(vox + d, V)))
                def _():
                    part_copy(t, d).start()
            if t:
                finish(t - 1)
    finish(T - 1)

    for local in range(SL):
        p = local * V + vox
        handler = lax.rem(p, G)
        for b in range(PG):
            source = (subj * PG + b) * VR

            @pl.when(jnp.logical_or(handler != subj, source != vox))
            def _():
                pltpu.make_async_remote_copy(
                    src_ref=summed.at[0], dst_ref=landed.at[local, b],
                    send_sem=fin_send.at[0], recv_sem=fin_recv.at[local, b],
                    device_id=(subj, lax.rem(vox + 1, V)),
                    device_id_type=pl.DeviceIdType.MESH,
                ).wait_recv()
            out_ref[local, b * RP:(b + 1) * RP] = landed[local, b]

    for h in range(H):
        for d in range(1, V):
            slab_copy(h, d, vox).wait_send()
        for i, n in groups(h):
            for d in range(1, G):
                score_copy(h, i, n, d, subj, every).wait_send()
    for t in range(T):
        for d in range(1, V):
            @pl.when(reduces(lax.rem(vox + d, V)))
            def _():
                part_copy(t, d).wait_send()

        @pl.when(jnp.logical_and(reduces(vox), away(t)))
        def _():
            final_copy(t).wait_send()


def body(series, offsets, selected):
    G = lax.axis_size("subj")
    V = lax.axis_size("vox")
    NS, RUN, VL = series.shape
    EP = offsets.shape[1]
    SEL = selected.shape[0]
    W = 256
    NE = NS * EP
    ROWS = EP * TR
    H = SEL // KB
    KH = KB // G
    SL = SEL // V
    R = pieces_of(G, V, NE)
    RP = G * NE // R
    vm = pltpu.VMEM
    dma = pltpu.SemaphoreType.DMA
    return pl.pallas_call(
        functools.partial(kernel, G, V, NS, EP, SEL, W),
        out_shape=jax.ShapeDtypeStruct((SL, NE, G * NE), f32),
        in_specs=[
            pl.BlockSpec(memory_space=pltpu.SMEM),
            pl.BlockSpec(memory_space=pltpu.SMEM),
            pl.BlockSpec(memory_space=pl.ANY),
        ],
        out_specs=pl.BlockSpec(memory_space=pltpu.VMEM),
        scratch_shapes=[
            vm((NS, RUN, VL), bf16),
            dma((NS,)),
            vm((NS, ROWS, VL), bf16),
            vm((NS, ROWS, RUN), bf16),
            vm((NS, EP, VL), f32),
            vm((H, KB, NS * ROWS), bf16),
            vm((H, V, KB, NS * ROWS), bf16),
            vm((H, NS, EP * KB, ROWS), bf16),
            vm((H, NS, EP * KB, ROWS), bf16),
            vm((KB * NE, KB * NE), bf16),
            vm((H, G, KH, NE, VL), bf16),
            vm((H, KH, G * NE, VL), bf16),
            vm((H * KH, G * NE, G * NE), f32),
            vm((H * KH, V - 1, RP, G * NE), f32),
            vm((H * KH, RP, G * NE), f32),
            vm((SL, R // G, RP, G * NE), f32),
            dma((H, V)),
            dma((H, V)),
            dma((H, KH, G)),
            dma((H, KH, G)),
            dma((H * KH, V)),
            dma((H * KH,)),
            dma((H * KH,)),
            dma((SL, R // G)),
        ],
        compiler_params=pltpu.CompilerParams(
            collective_id=0, has_side_effects=True, vmem_limit_bytes=56 * 1024 * 1024
        ),
    )(offsets, selected, series)


def solution(mesh):
    placed = (P("subj", None, "vox"), P(), P())
    return jax.shard_map(
        body, mesh=mesh, in_specs=placed, out_specs=P("vox", "subj", None), check_vma=False
    )
```

```python
import functools

import jax
import jax.numpy as jnp
from jax import lax
from jax.experimental import pallas as pl
from jax.experimental.pallas import tpu as pltpu
from jax.sharding import PartitionSpec as P

TR = 16
KB = 8
C1 = 4
series_floor = 1.0
spread_floor = 0.05
shrink_factor = 0.9
f32 = jnp.float32
bf16 = jnp.bfloat16


def iota(shape, dim):
    return lax.broadcasted_iota(jnp.int32, shape, dim)


def pieces_of(G, V, NE):
    R = V
    while R > G and (V % R or R % G or (G * NE) % R or (G * NE // R) % 8):
        R -= 1
    return R


def kernel(
    G, V, NS, EP, SEL, W,
    off_ref, sel_ref, series_hbm, out_ref,
    series_ref, load_sem, ep, hot, inv, part, slots, a_hi, a_lo, perm, send, recv,
    gram, pieces_in, summed, landed,
    slab_send, slab_recv, sc_send, sc_recv, rs_send, rs_recv, fin_send, fin_recv,
):
    subj = lax.axis_index("subj")
    vox = lax.axis_index("vox")
    RUN = series_ref.shape[1]
    VL = series_ref.shape[2]
    ROWS = EP * TR
    H = SEL // KB
    KH = KB // G
    SL = SEL // V
    NE = NS * EP
    chunks = VL // W
    R = pieces_of(G, V, NE)
    VR = V // R
    RP = G * NE // R
    PG = R // G
    ORDER = tuple(range(G // 2, G)) + tuple(range(1, G // 2))

    barrier = pltpu.get_barrier_semaphore()
    for d in range(1, G):
        pl.semaphore_signal(
            barrier, inc=1, device_id=(lax.rem(subj + d, G), vox),
            device_id_type=pl.DeviceIdType.MESH,
        )
    for d in range(1, V):
        pl.semaphore_signal(
            barrier, inc=1, device_id=(subj, lax.rem(vox + d, V)),
            device_id_type=pl.DeviceIdType.MESH,
        )

    def load(s):
        return pltpu.make_async_copy(series_hbm.at[s], series_ref.at[s], load_sem.at[s])

    for s in range(NS):
        load(s).start()

    ids = jnp.zeros((SEL, 1), jnp.int32)
    which = iota((SEL, 1), 0)
    for p in range(SEL):
        ids = jnp.where(which == p, sel_ref[(p % V) * SL + p // V], ids)
    picker = jnp.where(iota((SEL, VL), 1) + vox * VL == ids, 1.0, 0.0).astype(bf16)
    col = iota((TR, RUN), 1) - iota((TR, RUN), 0)
    pieces = []
    for s in range(NS):
        tiles = [
            jnp.where(col == off_ref[subj * NS + s, e], 1.0, 0.0) for e in range(EP)
        ]
        hot[s] = jnp.concatenate(tiles, axis=0).astype(bf16)
    for s in range(NS):
        load(s).wait()
        runs = lax.dot_general(
            picker, series_ref[s], (((1,), (1,)), ((), ())), preferred_element_type=f32
        )
        pieces.append(lax.dot_general(
            runs.astype(bf16), hot[s], (((1,), (1,)), ((), ())), preferred_element_type=f32
        ))
    joined = jnp.concatenate(pieces, axis=1)
    for h in range(H):
        part[h] = joined[h * KB:(h + 1) * KB].astype(bf16)

    def gather(c, carry):
        at = pl.ds(pl.multiple_of(c * W, W), W)
        for s in range(NS):
            x = jnp.dot(hot[s], series_ref[s, :, at], preferred_element_type=f32)
            ep[s, :, at] = x.astype(bf16)
            x3 = x.reshape(EP, TR, W)
            total = jnp.sum(x3, axis=1)
            ssq = jnp.sum(x3 * x3, axis=1) - total * total * (1.0 / TR)
            inv[s, :, at] = shrink_factor * lax.rsqrt(jnp.maximum(ssq, 0.0) + series_floor)
        return carry

    after = chunks * C1 // 8
    pl.semaphore_wait(barrier, G + V - 2)

    def slab_copy(h, d, sender):
        return pltpu.make_async_remote_copy(
            src_ref=part.at[h], dst_ref=slots.at[h, sender],
            send_sem=slab_send.at[h, d], recv_sem=slab_recv.at[h, d],
            device_id=(subj, lax.rem(vox + d, V)),
            device_id_type=pl.DeviceIdType.MESH,
        )

    for h in range(H):
        for d in range(1, V):
            slab_copy(h, d, vox).start()

    out_row = iota((KB * NE, KB * NE), 0)
    in_row = iota((KB * NE, KB * NE), 1)
    slot = out_row // NE
    source = lax.rem(out_row, NE) * KB + lax.rem(slot, KH) * G + slot // KH
    perm[...] = jnp.where(source == in_row, 1.0, 0.0).astype(bf16)

    lax.fori_loop(0, after, gather, 0)

    same = iota((ROWS, ROWS), 0) // TR == iota((ROWS, ROWS), 1) // TR
    ones = jnp.where(same, 1.0, 0.0)
    pick_e = iota((EP, KB, ROWS), 2) // TR == iota((EP, KB, ROWS), 0)

    def slab_rows(h):
        slab = part[h].astype(f32)
        for d in range(1, V):
            slab_copy(h, d, lax.rem(vox - d + V, V)).wait_recv()
        for d in range(1, V):
            slab = slab + slots[h, lax.rem(vox + d, V)].astype(f32)
        rows = jnp.concatenate(
            [slab[:, s * ROWS:(s + 1) * ROWS] for s in range(NS)], axis=0
        )
        mean = jnp.dot(
            rows.astype(bf16), ones.astype(bf16), preferred_element_type=f32
        ) * (1.0 / TR)
        centred = rows - mean
        ssq = jnp.dot(
            centred * centred, ones,
            precision=lax.Precision.HIGHEST, preferred_element_type=f32,
        )
        std = centred / jnp.sqrt(ssq + series_floor)
        hi = std.astype(bf16).astype(f32)
        lo = std - hi
        for s in range(NS):
            for value, where in ((hi, a_hi), (lo, a_lo)):
                block = value[s * KB:(s + 1) * KB]
                spread = jnp.where(pick_e, block[None], 0.0).reshape(EP * KB, ROWS)
                where[h, s] = spread.astype(bf16)

    every = pl.ds(0, VL)

    def score_copy(h, i, n, d, sender, at):
        return pltpu.make_async_remote_copy(
            src_ref=send.at[h, lax.rem(subj + d, G), pl.ds(i, n), :, at],
            dst_ref=recv.at[h, pl.ds(i, n), pl.ds(pl.multiple_of(sender * NE, NE), NE), at],
            send_sem=sc_send.at[h, i, d], recv_sem=sc_recv.at[h, i, d],
            device_id=(lax.rem(subj + d, G), vox),
            device_id_type=pl.DeviceIdType.MESH,
        )

    def groups(h):
        return ((0, KH),) if h == 0 else tuple((i, 1) for i in range(KH))

    own_rows = pl.ds(pl.multiple_of(subj * NE, NE), NE)
    for h in range(H):
        slab_rows(h)

        def scores(c, carry, h=h):
            if h == 0 and after < chunks:
                @pl.when(c >= after)
                def _():
                    gather(c, 0)

            at = pl.ds(pl.multiple_of(c * W, W), W)
            parts = []
            for s in range(NS):
                x = ep[s, :, at]
                corr = jnp.dot(a_hi[h, s], x, preferred_element_type=f32)
                corr = corr + jnp.dot(a_lo[h, s], x, preferred_element_type=f32)
                r = corr.reshape(EP, KB, W) * inv[s, :, at][:, None, :]
                f = 0.5 * (jnp.log(1.0 + r) - jnp.log(1.0 - r))
                f = f - jnp.sum(f, axis=0, keepdims=True) * (1.0 / EP)
                var = jnp.sum(f * f, axis=0, keepdims=True) * (1.0 / EP)
                z = f * lax.rsqrt(var + spread_floor)
                parts.append(z.reshape(EP * KB, W).astype(bf16))
            z = jnp.concatenate(parts, axis=0)
            moved = jnp.dot(perm[...], z, preferred_element_type=f32)
            send[h, :, :, :, at] = moved.astype(bf16).reshape(G, KH, NE, W)
            if h == 0:
                for d in ORDER:
                    score_copy(h, 0, KH, d, subj, at).start()
            recv[h, :, own_rows, at] = send[h, subj, :, :, at]
            return carry

        lax.fori_loop(0, chunks, scores, 0)

        if h:
            for i, n in groups(h):
                for d in ORDER:
                    score_copy(h, i, n, d, subj, every).start()

    def row_piece(r):
        return pl.ds(pl.multiple_of(r * RP, RP), RP)

    def part_copy(t, d):
        to = lax.rem(vox + d, V)
        return pltpu.make_async_remote_copy(
            src_ref=gram.at[t, row_piece(to // VR)], dst_ref=pieces_in.at[t, d - 1],
            send_sem=rs_send.at[t, d], recv_sem=rs_recv.at[t],
            device_id=(subj, to), device_id_type=pl.DeviceIdType.MESH,
        )

    def all_parts(t):
        return pltpu.make_async_remote_copy(
            src_ref=pieces_in.at[t], dst_ref=pieces_in.at[t],
            send_sem=rs_send.at[t, 0], recv_sem=rs_recv.at[t],
            device_id=(subj, lax.rem(vox + 1, V)), device_id_type=pl.DeviceIdType.MESH,
        )

    piece = vox // VR
    to_subj = piece // PG
    to_rows = lax.rem(piece, PG)

    def reduces(v):
        return lax.rem(v, VR) == 0

    def spot(t):
        p = t * G + subj
        return lax.rem(p, V), p // V

    def final_copy(t):
        owner, local = spot(t)
        return pltpu.make_async_remote_copy(
            src_ref=summed.at[t], dst_ref=landed.at[local, to_rows],
            send_sem=fin_send.at[t], recv_sem=fin_recv.at[local, to_rows],
            device_id=(to_subj, owner), device_id_type=pl.DeviceIdType.MESH,
        )

    def away(t):
        owner, local = spot(t)
        return jnp.logical_or(to_subj != subj, owner != vox)

    def finish(t):
        @pl.when(reduces(vox))
        def _():
            all_parts(t).wait_recv()
            total = gram[t, row_piece(piece)]
            for d in range(1, V):
                total = total + pieces_in[t, d - 1]
            total = total * (1.0 / (VL * V))
            summed[t] = total

            @pl.when(away(t))
            def _():
                final_copy(t).start()

            @pl.when(jnp.logical_not(away(t)))
            def _():
                landed[spot(t)[1], to_rows] = total

    T = H * KH
    for h in range(H):
        for i in range(KH):
            t = h * KH + i
            for first, n in groups(h):
                if first == i:
                    for d in range(1, G):
                        sender = lax.rem(subj - d + G, G)
                        score_copy(h, i, n, d, sender, every).wait_recv()
            rows = recv[h, i]
            gram[t] = lax.dot_general(
                rows, rows, (((1,), (1,)), ((), ())), preferred_element_type=f32
            )
            for d in range(1, V):
                @pl.when(reduces(lax.rem(vox + d, V)))
                def _():
                    part_copy(t, d).start()
            if t:
                finish(t - 1)
    finish(T - 1)

    for local in range(SL):
        p = local * V + vox
        handler = lax.rem(p, G)
        for b in range(PG):
            source = (subj * PG + b) * VR

            @pl.when(jnp.logical_or(handler != subj, source != vox))
            def _():
                pltpu.make_async_remote_copy(
                    src_ref=summed.at[0], dst_ref=landed.at[local, b],
                    send_sem=fin_send.at[0], recv_sem=fin_recv.at[local, b],
                    device_id=(subj, lax.rem(vox + 1, V)),
                    device_id_type=pl.DeviceIdType.MESH,
                ).wait_recv()
            out_ref[local, b * RP:(b + 1) * RP] = landed[local, b]

    for h in range(H):
        for d in range(1, V):
            slab_copy(h, d, vox).wait_send()
        for i, n in groups(h):
            for d in range(1, G):
                score_copy(h, i, n, d, subj, every).wait_send()
    for t in range(T):
        for d in range(1, V):
            @pl.when(reduces(lax.rem(vox + d, V)))
            def _():
                part_copy(t, d).wait_send()

        @pl.when(jnp.logical_and(reduces(vox), away(t)))
        def _():
            final_copy(t).wait_send()


def body(series, offsets, selected):
    G = lax.axis_size("subj")
    V = lax.axis_size("vox")
    NS, RUN, VL = series.shape
    EP = offsets.shape[1]
    SEL = selected.shape[0]
    W = 256
    NE = NS * EP
    ROWS = EP * TR
    H = SEL // KB
    KH = KB // G
    SL = SEL // V
    R = pieces_of(G, V, NE)
    RP = G * NE // R
    vm = pltpu.VMEM
    dma = pltpu.SemaphoreType.DMA
    return pl.pallas_call(
        functools.partial(kernel, G, V, NS, EP, SEL, W),
        out_shape=jax.ShapeDtypeStruct((SL, NE, G * NE), f32),
        in_specs=[
            pl.BlockSpec(memory_space=pltpu.SMEM),
            pl.BlockSpec(memory_space=pltpu.SMEM),
            pl.BlockSpec(memory_space=pl.ANY),
        ],
        out_specs=pl.BlockSpec(memory_space=pltpu.VMEM),
        scratch_shapes=[
            vm((NS, RUN, VL), bf16),
            dma((NS,)),
            vm((NS, ROWS, VL), bf16),
            vm((NS, ROWS, RUN), bf16),
            vm((NS, EP, VL), f32),
            vm((H, KB, NS * ROWS), bf16),
            vm((H, V, KB, NS * ROWS), bf16),
            vm((H, NS, EP * KB, ROWS), bf16),
            vm((H, NS, EP * KB, ROWS), bf16),
            vm((KB * NE, KB * NE), bf16),
            vm((H, G, KH, NE, VL), bf16),
            vm((H, KH, G * NE, VL), bf16),
            vm((H * KH, G * NE, G * NE), f32),
            vm((H * KH, V - 1, RP, G * NE), f32),
            vm((H * KH, RP, G * NE), f32),
            vm((SL, R // G, RP, G * NE), f32),
            dma((H, V)),
            dma((H, V)),
            dma((H, KH, G)),
            dma((H, KH, G)),
            dma((H * KH, V)),
            dma((H * KH,)),
            dma((H * KH,)),
            dma((SL, R // G)),
        ],
        compiler_params=pltpu.CompilerParams(
            collective_id=0, has_side_effects=True, vmem_limit_bytes=56 * 1024 * 1024
        ),
    )(offsets, selected, series)


def solution(mesh):
    placed = (P("subj", None, "vox"), P(), P())
    return jax.shard_map(
        body, mesh=mesh, in_specs=placed, out_specs=P("vox", "subj", None), check_vma=False
    )
```
